32 devices in a mesh: section: 4 (over z), dp: 8 (over y, x, core).
Axes of the slice: x: 2, y: 2, z: 4, core: 2. Of those that a mesh axis runs over, the one named last changes fastest.
Arguments:
- inputs: bfloat16 [2048, 2048], P('dp'), may hold values from -6 to 6
- order: int32 [8, 2], P('dp'), may hold values from 0 to 1, each once within a row
- image_start: int32 [8, 2], P('dp'), may hold values from 0 to 112, as said below
- image_len: int32 [8, 2], P('dp'), may hold values from 16 to 64
- norm_gain: float32 [4, 2048], P('section'), may hold values from 0.25 to 1.75
- qkv_weight: bfloat16 [4, 2048, 6144], P('section', 'dp'), may hold values from -0.125 to 0.125
- q_gain: float32 [4, 2048], P('section'), may hold values from 0.5 to 2.5
- k_gain: float32 [4, 2048], P('section'), may hold values from 0.5 to 2.5
- o_weight: bfloat16 [4, 2048, 2048], P('section'), may hold values from -0.125 to 0.125
Outputs:
- section_outputs: bfloat16 [4, 2048, 2048], P('section', 'dp')
The draws below stay inside these ranges and needn't reach their ends.
Inputs may be any that keep to these rules, and one draw needn't show every extreme that they name: `order`: each row is a permutation of the micro-batch numbers. image_start + image_len <= 128 for every micro-batch.
All inputs are finite; a program needn't handle non-finite values.
Results may differ from the reference program's by a relative error of at most 0.035.
Values may be sent and summed in bfloat16 or wider, within the bound.
A program may use at most 128 MiB of HBM per device.

```python
import math
import jax
import jax.numpy as jnp
from jax import lax

HEADS = 16
HEAD_DIM = 128
SEQ = 128
MICRO = 2
D = 2048
TOKENS = 2048
N_SECTION = 4
N_DP = 8


def span_pair(key):
    folded = jax.random.fold_in(key, 7)
    shortest = max(1, SEQ // 8)
    longest = SEQ // 2
    length = jax.random.randint(jax.random.fold_in(folded, 1), (N_DP, MICRO), shortest, longest + 1)
    random_bits = jax.random.randint(jax.random.fold_in(folded, 2), (N_DP, MICRO), 0, 1 << 20)
    chosen_group = jax.random.randint(jax.random.fold_in(folded, 3), (), 0, N_DP)
    chosen_micro = jax.random.randint(jax.random.fold_in(folded, 4), (), 0, MICRO)
    second_micro = (chosen_micro + 1) % MICRO
    group_index = jnp.arange(N_DP, dtype=jnp.int32)[:, None]
    micro_index = jnp.arange(MICRO, dtype=jnp.int32)[None, :]
    at_end = (group_index == chosen_group) & (micro_index == chosen_micro)
    at_long = (group_index == chosen_group) & (micro_index == second_micro)
    length = jnp.where(at_end, shortest, jnp.where(at_long, longest, length))
    start = random_bits % (SEQ - length + 1)
    start = jnp.where(at_end, SEQ - shortest, start)
    return (start.astype(jnp.int32), length.astype(jnp.int32))


def draw_image_start(key, part):
    return span_pair(key)[0]


def draw_image_len(key, part):
    return span_pair(key)[1]


def level_of(rng, shape, pieces, low, high):
    level, own = 1.0, jax.random.fold_in(rng, 6)
    for axis_at, shards_of in pieces:
        heights = jnp.exp(jax.random.uniform(jax.random.fold_in(own, axis_at), (shards_of,), jnp.float32, low / len(pieces), high / len(pieces)))
        level = level * jnp.repeat(heights, shape[axis_at] // shards_of).reshape([-1 if axis == axis_at else 1 for axis in range(len(shape))])
    return level


def scatter_about(stream_key, dims, deviation, most, cuts=(), kind=jnp.bfloat16):
    entries = deviation * jax.random.normal(stream_key, dims, jnp.float32)
    if cuts:
        entries = entries * level_of(stream_key, dims, cuts, -0.22, 0.18)
    return jnp.clip(entries, -most, most).astype(kind)


def setup_inputs(seed: int = 0) -> dict:
    keys = jax.random.split(jax.random.key(seed), 10)
    inputs = scatter_about(keys[0], (TOKENS, D), 1.0, 6.0, ((0, 8),))
    order = jax.vmap(lambda own: jax.random.permutation(own, MICRO))(jax.random.split(keys[1], N_DP)).reshape((N_DP, MICRO)).astype(jnp.int32)
    image_start = draw_image_start(jax.random.fold_in(keys[9], 71), 0)
    image_len = draw_image_len(jax.random.fold_in(keys[9], 71), 0)
    norm_gain = jnp.clip(1.0 + 0.15 * jax.random.normal(keys[4], (N_SECTION, D), jnp.float32), 0.25, 1.75)
    qkv_weight = scatter_about(keys[5], (N_SECTION, D, 3 * D), D ** -0.5, 0.125, ((0, 4), (1, 8)))
    q_gain = jnp.clip(jnp.exp(math.log(2.5) - 1.609438 * jax.random.uniform(keys[6], (N_SECTION, D), jnp.float32) ** level_of(keys[6], (N_SECTION, D), ((0, 4),), -0.2, 0.2)), 0.5, 2.5)
    k_gain = jnp.clip(jnp.exp(math.log(2.5) - 1.609438 * jax.random.uniform(keys[7], (N_SECTION, D), jnp.float32) ** level_of(keys[7], (N_SECTION, D), ((0, 4),), -0.2, 0.2)), 0.5, 2.5)
    o_weight = scatter_about(keys[8], (N_SECTION, D, D), D ** -0.5, 0.125, ((0, 4),))
    return dict(inputs=inputs, order=order, image_start=image_start, image_len=image_len, norm_gain=norm_gain, qkv_weight=qkv_weight, q_gain=q_gain, k_gain=k_gain, o_weight=o_weight)


epsilon_value = 1e-05

def normalize(hidden, gain):
    widened = hidden.astype(jnp.float32)
    mean_square = lax.optimization_barrier(jnp.mean(widened * widened, axis=-1, keepdims=True))
    return (widened * lax.rsqrt(mean_square + epsilon_value) * gain).astype(jnp.bfloat16)

def head_norm(block, gain, seq_len):
    split = block.reshape(seq_len, HEADS, HEAD_DIM)
    mean_square = lax.optimization_barrier(jnp.mean(split * split, axis=-1, keepdims=True))
    return (split * lax.rsqrt(mean_square + epsilon_value) * gain.reshape(HEADS, HEAD_DIM)).astype(jnp.bfloat16)

def finish(hidden, projected, gain_query, gain_key, out_weight, start, length):
    seq_len, model_width = hidden.shape
    queries = head_norm(projected[:, :model_width], gain_query, seq_len)
    key_rows = head_norm(projected[:, model_width:2 * model_width], gain_key, seq_len)
    value_rows = projected[:, 2 * model_width:].astype(jnp.bfloat16).reshape(seq_len, HEADS, HEAD_DIM)
    scores = jnp.einsum('qhd,khd->hqk', queries.astype(jnp.float32), key_rows.astype(jnp.float32)) * HEAD_DIM ** (-0.5)
    position = jnp.arange(seq_len, dtype=jnp.int32)
    in_image = (position >= start) & (position < start + length)
    allowed = (position[None, :] <= position[:, None]) | in_image[:, None] & in_image[None, :]
    scores = jnp.where(allowed[None], scores, -1e+30)
    row_max = lax.optimization_barrier(jnp.max(scores, axis=-1, keepdims=True))
    lifted = jnp.exp(scores - row_max)
    probabilities = (lifted / lax.optimization_barrier(jnp.sum(lifted, axis=-1, keepdims=True))).astype(jnp.bfloat16)
    mixed = jnp.einsum('hqk,khd->qhd', probabilities.astype(jnp.float32), value_rows.astype(jnp.float32))
    attended = mixed.reshape(seq_len, model_width).astype(jnp.bfloat16)
    output_rows = jnp.dot(attended, out_weight, preferred_element_type=jnp.float32)
    return (hidden.astype(jnp.float32) + output_rows).astype(jnp.bfloat16)

def reference(inputs, order, image_start, image_len, norm_gain, qkv_weight, q_gain, k_gain, o_weight):
    groups = inputs.reshape(N_DP, MICRO, SEQ, D)

    def one_group(packed):
        states, permutation, starts, lengths = packed
        states = states[permutation.astype(jnp.int32)]
        starts = starts[permutation.astype(jnp.int32)]
        lengths = lengths[permutation.astype(jnp.int32)]
        collected = []
        for section_number in range(N_SECTION):
            normed = normalize(states.reshape(MICRO * SEQ, D), norm_gain[section_number])
            projected = jnp.dot(normed, qkv_weight[section_number], preferred_element_type=jnp.float32)
            projected = projected.reshape(MICRO, SEQ, 3 * D)
            gain_query = q_gain[section_number]
            gain_key = k_gain[section_number]
            out_weight = o_weight[section_number]
            states = jax.vmap(lambda one, proj_rows, first, count: finish(one, proj_rows, gain_query, gain_key, out_weight, first, count))(states, projected, starts, lengths)
            collected.append(states)
        return jnp.stack(collected)
    result = lax.map(one_group, (groups, order, image_start, image_len))
    return jnp.transpose(result, (1, 0, 2, 3, 4)).reshape(N_SECTION, N_DP * MICRO * SEQ, D)
```

```python
import functools
import jax
import jax.numpy as jnp
from jax import lax
from jax.experimental import pallas as pl
from jax.experimental.pallas import tpu as pltpu
from jax.sharding import PartitionSpec as P

HEAD_DIM = 128
EPS = 1e-05
SUBS = 2
MESH = pl.DeviceIdType.MESH


def ring_order(chips):
    columns = 1
    while columns * columns < chips:
        columns *= 2
    rows = chips // columns
    cells = []
    for r in range(rows):
        line = list(range(1, columns))
        cells += [r * columns + c for c in (line if r % 2 == 0 else line[::-1])]
    cells += [r * columns for r in reversed(range(rows))]
    return cells


def look(table, index):
    found = jnp.int32(0)
    for i, value in enumerate(table):
        found = found + jnp.where(index == i, jnp.int32(value), jnp.int32(0))
    return found


def kernel(
    sections, devices, tile,
    order_ref, start_ref, len_ref, x_ref, gain_ref, w_ref, qg_ref, kg_ref, o_ref,
    out_ref,
    wbuf, obuf, xin, xout, acc, qkv, att,
    own_sem, o_sem, first_send, first_recv, ring_send, ring_recv, pair_send, pair_recv,
    hop_send, hop_recv,
):
    chips = devices // 2
    order = ring_order(chips)
    inverse = [order.index(c) for c in range(chips)]
    shard = w_ref.shape[0]
    piece = shard // (2 * SUBS)
    micro, chunks, seq, width = xin.shape
    model = chunks * width
    sec = lax.axis_index("section")
    me = lax.axis_index("dp")
    core = lax.rem(me, 2)
    place = look(inverse, me // 2)
    partner = me + 1 - 2 * core

    def at(offset):
        return look(order, lax.rem(place + (offset % chips), chips)) * 2 + core

    ahead, behind = at(1), at(-1)
    above = lax.rem(sec + 1, sections)
    below = lax.rem(sec + sections - 1, sections)

    barrier = pltpu.get_barrier_semaphore()
    for other in ((sec, ahead), (sec, behind), (sec, partner), (above, me), (below, me)):
        pl.semaphore_signal(barrier, inc=1, device_id=other, device_id_type=MESH)
    pl.semaphore_wait(barrier, 5)

    own_rows = pl.ds(pl.multiple_of(me * shard, shard), shard)

    def rows(owner, way, sub):
        return pl.ds(pl.multiple_of(owner * shard + (way * SUBS + sub) * piece, piece), piece)

    def ring_copy(way, sub, step):
        owner = at(-step if way == 0 else step)
        where = rows(owner, way, sub)
        if step == 0:
            source = w_ref.at[pl.ds((way * SUBS + sub) * piece, piece)]
        else:
            source = wbuf.at[where]
        return pltpu.make_async_remote_copy(
            src_ref=source, dst_ref=wbuf.at[where],
            send_sem=ring_send.at[way, sub, step], recv_sem=ring_recv.at[way, sub, step],
            device_id=(sec, ahead if way == 0 else behind), device_id_type=MESH,
        )

    def pair_copy(way, sub, step):
        owner = at(-step if way == 0 else step)
        where = rows(owner, way, sub)
        return pltpu.make_async_remote_copy(
            src_ref=wbuf.at[where], dst_ref=wbuf.at[where],
            send_sem=pair_send.at[way, sub, step - 1], recv_sem=pair_recv.at[way, sub, step - 1],
            device_id=(sec, partner), device_id_type=MESH,
        )

    ring = {}
    pair = {}
    for sub in range(SUBS):
        for way in range(2):
            ring[way, sub, 0] = ring_copy(way, sub, 0)
            ring[way, sub, 0].start()
    first = pltpu.make_async_remote_copy(
        src_ref=w_ref, dst_ref=wbuf.at[own_rows], send_sem=first_send, recv_sem=first_recv,
        device_id=(sec, partner), device_id_type=MESH,
    )
    first.start()
    own = pltpu.make_async_copy(w_ref, wbuf.at[own_rows], own_sem)
    own.start()
    o_copy = pltpu.make_async_copy(o_ref, obuf, o_sem)
    o_copy.start()
    for step in range(1, chips):
        for sub in range(SUBS):
            for way in range(2):
                ring[way, sub, step - 1].wait_recv()
                if step < chips - 1:
                    ring[way, sub, step] = ring_copy(way, sub, step)
                    ring[way, sub, step].start()
                pair[way, sub, step] = pair_copy(way, sub, step)
                pair[way, sub, step].start()
    own.wait()
    o_copy.wait()
    first.wait()
    for step in range(1, chips):
        for sub in range(SUBS):
            for way in range(2):
                pair[way, sub, step].wait()
                ring[way, sub, step - 1].wait_send()

    def hop(j, c):
        return pltpu.make_async_remote_copy(
            src_ref=xout.at[j, c], dst_ref=xin.at[j, c],
            send_sem=hop_send.at[j, c], recv_sem=hop_recv.at[j, c],
            device_id=(above, me), device_id_type=MESH,
        )

    total = w_ref.shape[1]
    row_id = lax.broadcasted_iota(jnp.int32, (seq, seq), 0)
    col_id = lax.broadcasted_iota(jnp.int32, (seq, seq), 1)
    per_tile = tile // HEAD_DIM

    @pl.loop(0, micro)
    def _(j):
        which = order_ref[0, j]
        s0 = start_ref[0, which]
        s1 = s0 + len_ref[0, which]

        square = jnp.zeros((seq, 1), jnp.float32)
        for c in range(chunks):
            span = slice(c * width, (c + 1) * width)

            @pl.when(sec == 0)
            def _():
                xin[j, c] = x_ref[which, :, span]

            @pl.when(sec > 0)
            def _():
                hop(j, c).wait_recv()

            wide = xin[j, c].astype(jnp.float32)
            square = square + jnp.sum(wide * wide, axis=-1, keepdims=True)
            scaled = (wide * gain_ref[:, span]).astype(jnp.bfloat16)

            @pl.loop(0, total // tile)
            def _(n):
                cols = pl.ds(pl.multiple_of(n * tile, tile), tile)
                part = jnp.dot(scaled, wbuf[span, cols], preferred_element_type=jnp.float32)
                if c == 0:
                    acc[:, cols] = part
                else:
                    acc[:, cols] += part

        scale = lax.rsqrt(square * (1.0 / model) + EPS)

        for part, gains in ((0, qg_ref), (1, kg_ref)):
            @pl.loop(0, model // tile)
            def _(n):
                for i in range(per_tile):
                    here = pl.ds(pl.multiple_of(n * tile + i * HEAD_DIM, HEAD_DIM), HEAD_DIM)
                    cols = pl.ds(
                        pl.multiple_of(part * model + n * tile + i * HEAD_DIM, HEAD_DIM), HEAD_DIM
                    )
                    p = acc[:, cols] * scale
                    mean = jnp.mean(p * p, axis=-1, keepdims=True)
                    qkv[:, cols] = (p * lax.rsqrt(mean + EPS) * gains[:, here]).astype(jnp.bfloat16)

        allowed = (col_id <= row_id) | (
            (row_id >= s0) & (row_id < s1) & (col_id >= s0) & (col_id < s1)
        )

        @pl.loop(0, model // tile)
        def _(n):
            for i in range(per_tile):
                base = n * tile + i * HEAD_DIM
                here = pl.ds(pl.multiple_of(base, HEAD_DIM), HEAD_DIM)
                q = qkv[:, here]
                k = qkv[:, pl.ds(pl.multiple_of(model + base, HEAD_DIM), HEAD_DIM)]
                v = acc[:, pl.ds(pl.multiple_of(2 * model + base, HEAD_DIM), HEAD_DIM)] * scale
                scores = lax.dot_general(
                    q, k, (((1,), (1,)), ((), ())), preferred_element_type=jnp.float32
                ) * HEAD_DIM ** (-0.5)
                scores = jnp.where(allowed, scores, -1e30)
                lifted = jnp.exp(scores - jnp.max(scores, axis=-1, keepdims=True))
                weights = lifted / jnp.sum(lifted, axis=-1, keepdims=True)
                att[:, here] = jnp.dot(
                    weights.astype(jnp.bfloat16), v.astype(jnp.bfloat16),
                    preferred_element_type=jnp.float32,
                ).astype(jnp.bfloat16)

        for c in range(chunks):
            span = slice(c * width, (c + 1) * width)
            grown = jnp.dot(att[...], obuf[:, span], preferred_element_type=jnp.float32)
            fresh = (xin[j, c].astype(jnp.float32) + grown).astype(jnp.bfloat16)
            xout[j, c] = fresh
            out_ref[j, :, span] = fresh

            @pl.when(sec < sections - 1)
            def _():
                hop(j, c).start()

    @pl.when(sec < sections - 1)
    def _():
        for j in range(micro):
            for c in range(chunks):
                hop(j, c).wait_send()


def solution(mesh):
    sections, devices = mesh.shape["section"], mesh.shape["dp"]

    def body(inputs, order, image_start, image_len, norm_gain, qkv_weight, q_gain, k_gain, o_weight):
        micro = order.shape[1]
        count, model = inputs.shape
        seq = count // micro
        total = qkv_weight.shape[2]
        shard = qkv_weight.shape[1]
        width = tile = model // 4
        chunks = model // width
        chips = devices // 2
        smem = pl.BlockSpec(memory_space=pltpu.SMEM)
        vmem = pl.BlockSpec(memory_space=pltpu.VMEM)
        hbm = pl.BlockSpec(memory_space=pltpu.HBM)
        dma = pltpu.SemaphoreType.DMA
        out = pl.pallas_call(
            functools.partial(kernel, sections, devices, tile),
            out_shape=jax.ShapeDtypeStruct((micro, seq, model), jnp.bfloat16),
            in_specs=[smem, smem, smem, vmem, vmem, hbm, vmem, vmem, hbm],
            out_specs=vmem,
            scratch_shapes=[
                pltpu.VMEM((model, total), jnp.bfloat16),
                pltpu.VMEM((model, model), jnp.bfloat16),
                pltpu.VMEM((micro, chunks, seq, width), jnp.bfloat16),
                pltpu.VMEM((micro, chunks, seq, width), jnp.bfloat16),
                pltpu.VMEM((seq, total), jnp.float32),
                pltpu.VMEM((seq, 2 * model), jnp.bfloat16),
                pltpu.VMEM((seq, model), jnp.bfloat16),
                dma, dma, dma, dma,
                dma((2, SUBS, chips - 1)),
                dma((2, SUBS, chips - 1)),
                dma((2, SUBS, chips - 1)),
                dma((2, SUBS, chips - 1)),
                dma((micro, chunks)),
                dma((micro, chunks)),
            ],
            compiler_params=pltpu.CompilerParams(
                collective_id=0, has_side_effects=True, vmem_limit_bytes=60 * 1024 * 1024
            ),
        )(
            order, image_start, image_len, inputs.reshape(micro, seq, model), norm_gain,
            qkv_weight.reshape(shard, total), q_gain, k_gain, o_weight.reshape(model, model),
        )
        return out.reshape(1, count, model)

    in_specs = (
        P("dp", None),
        P("dp", None),
        P("dp", None),
        P("dp", None),
        P("section", None),
        P("section", "dp", None),
        P("section", None),
        P("section", None),
        P("section", None, None),
    )
    out_specs = P("section", "dp", None)
    return jax.shard_map(body, mesh=mesh, in_specs=in_specs, out_specs=out_specs, check_vma=False)
```

```python
import functools
import jax
import jax.numpy as jnp
from jax import lax
from jax.experimental import pallas as pl
from jax.experimental.pallas import tpu as pltpu
from jax.sharding import PartitionSpec as P

HEAD_DIM = 128
EPS = 1e-05
LOG2_E = 1.4426950408889634
SUBS = 2
CHUNKS = 4
WIDE = 1
EARLY_WIDE = 3
HEADS_AT_ONCE = 16
NORMS_AT_ONCE = 16
MESH = pl.DeviceIdType.MESH


def ring_order(chips):
    columns = 1
    while columns * columns < chips:
        columns *= 2
    rows = chips // columns
    cells = []
    for r in range(rows):
        line = list(range(1, columns))
        cells += [r * columns + c for c in (line if r % 2 == 0 else line[::-1])]
    cells += [r * columns for r in reversed(range(rows))]
    return cells


def look(table, index):
    found = jnp.int32(0)
    for i, value in enumerate(table):
        found = found + jnp.where(index == i, jnp.int32(value), jnp.int32(0))
    return found


def kernel(
    sections, devices,
    order_ref, start_ref, len_ref, x_ref, gain_ref, w_ref, qg_ref, kg_ref, o_ref,
    out_ref,
    wbuf, obuf, xin, xout, acc, qkv, att, early,
    own_sem, o_sem, first_send, first_recv, ring_send, ring_recv, pair_send, pair_recv,
    hop_send, hop_recv,
):
    chips = devices // 2
    order = ring_order(chips)
    inverse = [order.index(c) for c in range(chips)]
    shard = w_ref.shape[0]
    piece = shard // (2 * SUBS)
    micro, chunks, seq, width = xin.shape
    model = chunks * width
    sec = lax.axis_index("section")
    me = lax.axis_index("dp")
    core = lax.rem(me, 2)
    place = look(inverse, me // 2)
    partner = me + 1 - 2 * core

    def at(offset):
        return look(order, lax.rem(place + (offset % chips), chips)) * 2 + core

    ahead, behind = at(1), at(-1)
    above = lax.rem(sec + 1, sections)
    below = lax.rem(sec + sections - 1, sections)

    barrier = pltpu.get_barrier_semaphore()
    for other in ((sec, ahead), (sec, behind), (sec, partner), (above, me), (below, me)):
        pl.semaphore_signal(barrier, inc=1, device_id=other, device_id_type=MESH)
    pl.semaphore_wait(barrier, 5)

    own_rows = pl.ds(pl.multiple_of(me * shard, shard), shard)

    def rows(owner, way, sub):
        return pl.ds(pl.multiple_of(owner * shard + (way * SUBS + sub) * piece, piece), piece)

    def ring_copy(way, sub, step):
        owner = at(-step if way == 0 else step)
        where = rows(owner, way, sub)
        if step == 0:
            source = w_ref.at[pl.ds((way * SUBS + sub) * piece, piece)]
        else:
            source = wbuf.at[where]
        return pltpu.make_async_remote_copy(
            src_ref=source, dst_ref=wbuf.at[where],
            send_sem=ring_send.at[way, sub, step], recv_sem=ring_recv.at[way, sub, step],
            device_id=(sec, ahead if way == 0 else behind), device_id_type=MESH,
        )

    def pair_copy(way, sub, step):
        owner = at(-step if way == 0 else step)
        where = rows(owner, way, sub)
        return pltpu.make_async_remote_copy(
            src_ref=wbuf.at[where], dst_ref=wbuf.at[where],
            send_sem=pair_send.at[way, sub, step - 1], recv_sem=pair_recv.at[way, sub, step - 1],
            device_id=(sec, partner), device_id_type=MESH,
        )

    ring = {}
    pair = {}
    for sub in range(SUBS):
        for way in range(2):
            ring[way, sub, 0] = ring_copy(way, sub, 0)
            ring[way, sub, 0].start()
    first = pltpu.make_async_remote_copy(
        src_ref=w_ref, dst_ref=wbuf.at[own_rows], send_sem=first_send, recv_sem=first_recv,
        device_id=(sec, partner), device_id_type=MESH,
    )
    first.start()
    own = pltpu.make_async_copy(w_ref, wbuf.at[own_rows], own_sem)
    own.start()
    o_copy = pltpu.make_async_copy(o_ref, obuf, o_sem)
    o_copy.start()
    total = w_ref.shape[1]
    half = shard // 2

    @pl.when(sec == 0)
    def _():
        for j in range(micro):
            for n in range(model // half):
                part = x_ref[order_ref[0, j], :, n * half : (n + 1) * half].astype(jnp.float32)
                early[n, j * seq : (j + 1) * seq] = (
                    part * gain_ref[:, n * half : (n + 1) * half]
                ).astype(jnp.bfloat16)

    def absorb(halves, fresh=False):
        @pl.when(sec == 0)
        def _():
            @pl.loop(0, EARLY_WIDE)
            def _(n):
                cols = pl.ds(pl.multiple_of(n * (total // EARLY_WIDE), total // EARLY_WIDE), total // EARLY_WIDE)
                left = [early[h] for h in halves]
                right = [wbuf[pl.ds(pl.multiple_of(h * half, half), half), cols] for h in halves]
                if half % 128 == 0:
                    left = [jnp.concatenate(left, axis=1)]
                    right = [jnp.concatenate(right, axis=0)]
                for i, (one, other) in enumerate(zip(left, right)):
                    part = jnp.dot(one, other, preferred_element_type=jnp.float32)
                    if fresh and i == 0:
                        acc[:, cols] = part
                    else:
                        acc[:, cols] += part

    def mate(owner):
        return owner + 1 - 2 * core

    own.wait()
    first.wait_recv()
    absorb([2 * me, 2 * me + 1], fresh=True)
    absorb([2 * partner, 2 * partner + 1])
    for step in range(1, chips):
        for sub in range(SUBS):
            for way in range(2):
                ring[way, sub, step - 1].wait_recv()
                if step < chips - 1:
                    ring[way, sub, step] = ring_copy(way, sub, step)
                    ring[way, sub, step].start()
                pair[way, sub, step] = pair_copy(way, sub, step)
                pair[way, sub, step].start()
        for way in range(2):
            for sub in range(SUBS):
                pair[way, sub, step].wait_recv()
            owner = at(-step if way == 0 else step)
            absorb([2 * owner + way, 2 * mate(owner) + way])
    o_copy.wait()
    first.wait_send()
    for step in range(1, chips):
        for sub in range(SUBS):
            for way in range(2):
                pair[way, sub, step].wait_send()
                ring[way, sub, step - 1].wait_send()

    def hop(j, c):
        return pltpu.make_async_remote_copy(
            src_ref=xout.at[j, c], dst_ref=xin.at[j, c],
            send_sem=hop_send.at[j, c], recv_sem=hop_recv.at[j, c],
            device_id=(above, me), device_id_type=MESH,
        )

    row_id = lax.broadcasted_iota(jnp.int32, (seq, seq), 0)
    col_id = lax.broadcasted_iota(jnp.int32, (seq, seq), 1)

    @pl.loop(0, micro)
    def _(j):
        which = order_ref[0, j]
        s0 = start_ref[0, which]
        s1 = s0 + len_ref[0, which]

        own_seq = pl.ds(pl.multiple_of(j * seq, seq), seq)
        square = jnp.zeros((seq, 1), jnp.float32)
        for c in range(chunks):
            span = slice(c * width, (c + 1) * width)

            @pl.when(sec == 0)
            def _():
                xin[j, c] = x_ref[which, :, span]

            @pl.when(sec > 0)
            def _():
                hop(j, c).wait_recv()

            wide = xin[j, c].astype(jnp.float32)
            square = square + jnp.sum(wide * wide, axis=-1, keepdims=True)
            scaled = (wide * gain_ref[:, span]).astype(jnp.bfloat16)

            @pl.when(sec > 0)
            def _():
                @pl.loop(0, WIDE)
                def _(n):
                    cols = pl.ds(pl.multiple_of(n * (total // WIDE), total // WIDE), total // WIDE)
                    part = jnp.dot(scaled, wbuf[span, cols], preferred_element_type=jnp.float32)
                    if c == 0:
                        acc[own_seq, cols] = part
                    else:
                        acc[own_seq, cols] += part

        scale = lax.rsqrt(square * (1.0 / model) + EPS)

        for part, gains in ((0, qg_ref), (1, kg_ref)):
            factor = HEAD_DIM ** (-0.5) * LOG2_E if part == 0 else 1.0

            @pl.loop(0, model // (NORMS_AT_ONCE * HEAD_DIM))
            def _(n):
                for i in range(NORMS_AT_ONCE):
                    base = (n * NORMS_AT_ONCE + i) * HEAD_DIM
                    here = pl.ds(pl.multiple_of(base, HEAD_DIM), HEAD_DIM)
                    cols = pl.ds(pl.multiple_of(part * model + base, HEAD_DIM), HEAD_DIM)
                    p = acc[own_seq, cols]
                    mean = jnp.mean(p * p, axis=-1, keepdims=True) * scale * scale
                    lift = lax.rsqrt(mean + EPS) * scale
                    qkv[:, cols] = (p * lift * (gains[:, here] * factor)).astype(jnp.bfloat16)

        allowed = (col_id <= row_id) | (
            (row_id >= s0) & (row_id < s1) & (col_id >= s0) & (col_id < s1)
        )

        @pl.loop(0, model // (HEADS_AT_ONCE * HEAD_DIM))
        def _(n):
            for i in range(HEADS_AT_ONCE):
                base = (n * HEADS_AT_ONCE + i) * HEAD_DIM
                here = pl.ds(pl.multiple_of(base, HEAD_DIM), HEAD_DIM)
                q = qkv[:, here]
                k = qkv[:, pl.ds(pl.multiple_of(model + base, HEAD_DIM), HEAD_DIM)]
                v = acc[own_seq, pl.ds(pl.multiple_of(2 * model + base, HEAD_DIM), HEAD_DIM)] * scale
                scores = lax.dot_general(
                    q, k, (((1,), (1,)), ((), ())), preferred_element_type=jnp.float32
                )
                lifted = jnp.where(allowed, jnp.exp2(scores), 0.0)
                mixed = jnp.dot(
                    lifted.astype(jnp.bfloat16), v.astype(jnp.bfloat16),
                    preferred_element_type=jnp.float32,
                )
                share = 1.0 / jnp.sum(lifted, axis=-1, keepdims=True)
                att[:, here] = (mixed * share).astype(jnp.bfloat16)

        for c in range(chunks):
            span = slice(c * width, (c + 1) * width)
            grown = jnp.dot(att[...], obuf[:, span], preferred_element_type=jnp.float32)
            fresh = (xin[j, c].astype(jnp.float32) + grown).astype(jnp.bfloat16)
            xout[j, c] = fresh
            out_ref[j, :, span] = fresh

            @pl.when(sec < sections - 1)
            def _():
                hop(j, c).start()

    @pl.when(sec < sections - 1)
    def _():
        for j in range(micro):
            for c in range(chunks):
                hop(j, c).wait_send()


def solution(mesh):
    sections, devices = mesh.shape["section"], mesh.shape["dp"]

    def body(inputs, order, image_start, image_len, norm_gain, qkv_weight, q_gain, k_gain, o_weight):
        micro = order.shape[1]
        count, model = inputs.shape
        seq = count // micro
        total = qkv_weight.shape[2]
        shard = qkv_weight.shape[1]
        width = model // CHUNKS
        chunks = model // width
        chips = devices // 2
        smem = pl.BlockSpec(memory_space=pltpu.SMEM)
        vmem = pl.BlockSpec(memory_space=pltpu.VMEM)
        hbm = pl.BlockSpec(memory_space=pltpu.HBM)
        dma = pltpu.SemaphoreType.DMA
        out = pl.pallas_call(
            functools.partial(kernel, sections, devices),
            out_shape=jax.ShapeDtypeStruct((micro, seq, model), jnp.bfloat16),
            in_specs=[smem, smem, smem, vmem, vmem, hbm, vmem, vmem, hbm],
            out_specs=vmem,
            scratch_shapes=[
                pltpu.VMEM((model, total), jnp.bfloat16),
                pltpu.VMEM((model, model), jnp.bfloat16),
                pltpu.VMEM((micro, chunks, seq, width), jnp.bfloat16),
                pltpu.VMEM((micro, chunks, seq, width), jnp.bfloat16),
                pltpu.VMEM((count, total), jnp.float32),
                pltpu.VMEM((seq, 2 * model), jnp.bfloat16),
                pltpu.VMEM((seq, model), jnp.bfloat16),
                pltpu.VMEM((2 * model // shard, count, shard // 2), jnp.bfloat16),
                dma, dma, dma, dma,
                dma((2, SUBS, chips - 1)),
                dma((2, SUBS, chips - 1)),
                dma((2, SUBS, chips - 1)),
                dma((2, SUBS, chips - 1)),
                dma((micro, chunks)),
                dma((micro, chunks)),
            ],
            compiler_params=pltpu.CompilerParams(
                collective_id=0, has_side_effects=True, vmem_limit_bytes=60 * 1024 * 1024
            ),
        )(
            order, image_start, image_len, inputs.reshape(micro, seq, model), norm_gain,
            qkv_weight.reshape(shard, total), q_gain, k_gain, o_weight.reshape(model, model),
        )
        return out.reshape(1, count, model)

    in_specs = (
        P("dp", None),
        P("dp", None),
        P("dp", None),
        P("dp", None),
        P("section", None),
        P("section", "dp", None),
        P("section", None),
        P("section", None),
        P("section", None, None),
    )
    out_specs = P("section", "dp", None)
    return jax.shard_map(body, mesh=mesh, in_specs=in_specs, out_specs=out_specs, check_vma=False)
```
